32 devices in a mesh: groups: 2 (over x), seq: 16 (over z, y, core).
Axes of the slice: x: 2, y: 2, z: 4, core: 2. Of those that a mesh axis runs over, the one named last changes fastest.
Arguments:
- attn_query: bfloat16 [8192, 2048], P(('groups', 'seq')), parts along dimension 0, may hold values from -16 to 16
- attn_key: bfloat16 [8192, 2048], P(('groups', 'seq')), parts along dimension 0, may hold values from -16 to 16
- attn_value: bfloat16 [8192, 2048], P(('groups', 'seq')), parts along dimension 0, may hold values from -6 to 6
- mesa_query: bfloat16 [8192, 2048], P(('groups', 'seq')), parts along dimension 0, may hold values from -6 to 6
- mesa_key: bfloat16 [8192, 2048], P(('groups', 'seq')), parts along dimension 0, may hold values from -16 to 16
- log_decay: float32 [8192, 16], P(('groups', 'seq')), parts along dimension 0, may hold values from -1 to 0
- input_gate: float32 [8192, 16], P(('groups', 'seq')), parts along dimension 0, may hold values from 0.2 to 1
- regularizer: float32 [16, 128], replicated, may hold values from 0.5 to 4
Outputs:
- attention: bfloat16 [8192, 2048], P(('groups', 'seq')), parts along dimension 0
- mesa_out: bfloat16 [8192, 2048], P(('groups', 'seq')), parts along dimension 0
The draws below stay inside these ranges and needn't reach their ends.
There are 2 independent parts, one for each index of `groups`. The reference program is written for one: setup_inputs(seed, part) draws one part's arguments, and reference() takes and returns one part's arrays. A program takes and returns all parts, laid end to end along the dimension named above; an argument that names none is the same for every part. Nothing has to cross between parts.
All inputs are finite; a program needn't handle non-finite values.
Results may differ from the reference program's by a relative error of at most 0.017.
Values may be sent and summed in bfloat16 or wider, within the bound.
No kernel may reach another device: no remote copies, remote signals or barrier semaphores. Data moves between devices by JAX's collectives and lax.ppermute only.
A program may use at most 128 MiB of HBM per device.

```python
import math
import jax
import jax.numpy as jnp
from jax import lax

HEAD_GROUP = 16
DK = 128
FEATURES = 2048
WINDOW = 2048
SPAN = 64
CG_ITERS = 8
TOK_DEV = 256
TOKEN_LENGTH = 4096


def drawn_pair(key):
    random_seeds = jax.random.split(jax.random.fold_in(key, 11), 2)
    base_query = jnp.clip(jax.random.normal(random_seeds[0], (TOKEN_LENGTH, FEATURES), jnp.float32), -4.0, 4.0)
    base_key = jnp.clip(jax.random.normal(random_seeds[1], (TOKEN_LENGTH, FEATURES), jnp.float32), -4.0, 4.0)
    return (base_query, base_key)


def draw_attn_query(key, part):
    return drawn_pair(key)[0].astype(jnp.bfloat16)


def draw_attn_key(key, part):
    return drawn_pair(key)[1].astype(jnp.bfloat16)


def draw_mesa_key(key, part):
    random_seeds = jax.random.split(jax.random.fold_in(key, 29), 3)
    overall = math.sqrt(32.0 / TOKEN_LENGTH)
    entries = jnp.clip(jax.random.normal(random_seeds[0], (TOKEN_LENGTH, FEATURES), jnp.float32), -4.0, 4.0)
    column = jnp.exp(jax.random.uniform(random_seeds[1], (1, FEATURES), jnp.float32, math.log(0.3), math.log(1.5)))
    coarse_result = jax.random.uniform(random_seeds[2], (TOKEN_LENGTH, 1), jnp.float32, 0.5, 1.5)
    return (entries * column * coarse_result * overall).astype(jnp.bfloat16)


def draw_log_decay(key, part):
    random_seeds = jax.random.split(jax.random.fold_in(key, 37), 7)
    share = 0.5
    slow = jax.random.uniform(random_seeds[0], (HEAD_GROUP,), jnp.float32) < share
    slow_rate = jax.random.uniform(random_seeds[1], (HEAD_GROUP,), jnp.float32, 0.1, 0.25) * math.log(10.0) / TOKEN_LENGTH
    fast_rate = math.log(10.0) / jax.random.uniform(random_seeds[2], (HEAD_GROUP,), jnp.float32, 30.0, 50.0)
    head_decay_rate = jnp.where(slow, slow_rate, fast_rate)
    slab_factor = jnp.exp(jax.random.uniform(random_seeds[3], (TOKEN_LENGTH // TOK_DEV, HEAD_GROUP), jnp.float32, math.log(0.5), math.log(2.0)))
    piece_rows = jnp.repeat(slab_factor, TOK_DEV, axis=0)
    coarse_result = jax.random.uniform(random_seeds[4], (TOKEN_LENGTH, HEAD_GROUP), jnp.float32, 0.5, 1.5)
    segment_list = jax.random.randint(random_seeds[5], (2,), 0, TOKEN_LENGTH)
    segment_rows = jnp.any(jnp.arange(TOKEN_LENGTH)[:, None] == segment_list[None, :], axis=1)[:, None]
    segment_loss = jnp.log(jax.random.uniform(random_seeds[6], (1, HEAD_GROUP), jnp.float32, 0.5, 0.8))
    return -(head_decay_rate[None, :] * piece_rows * coarse_result) + jnp.where(segment_rows, segment_loss, 0.0)


def block_scale(rng, shape, cuts, smallest, largest):
    loudness, own = 1.0, jax.random.fold_in(rng, 6)
    for position, shards_of in cuts:
        draws = jnp.exp(jax.random.uniform(jax.random.fold_in(own, position), (shards_of,), jnp.float32, smallest / len(cuts), largest / len(cuts)))
        loudness = loudness * jnp.repeat(draws, shape[position] // shards_of).reshape([-1 if axis == position else 1 for axis in range(len(shape))])
    return loudness


def scatter_about(rng, extent, deviation, bound, cuts=(), kind=jnp.bfloat16):
    level = block_scale(rng, extent, cuts, -0.22, 0.18) if cuts else 1.0
    values = jax.random.normal(rng, extent, jnp.float32) * deviation * level
    return jnp.minimum(jnp.maximum(values, -bound), bound).astype(kind)


def setup_inputs(seed: int = 0, part: int = 0) -> dict:
    arg_keys = jax.random.split(jax.random.key(seed), 9)
    part_splits = jax.random.split(jax.random.fold_in(arg_keys[8], part), 9)
    attn_query = draw_attn_query(jax.random.fold_in(jax.random.fold_in(arg_keys[8], part), 71), part)
    attn_key = draw_attn_key(jax.random.fold_in(jax.random.fold_in(arg_keys[8], part), 71), part)
    attn_value = scatter_about(part_splits[2], (TOKEN_LENGTH, FEATURES), 1.0, 6.0, ((0, 16),))
    mesa_query = scatter_about(part_splits[3], (TOKEN_LENGTH, FEATURES), 1.0, 6.0, ((0, 16),))
    mesa_key = draw_mesa_key(jax.random.fold_in(jax.random.fold_in(arg_keys[8], part), 71), part)
    log_decay = draw_log_decay(jax.random.fold_in(jax.random.fold_in(arg_keys[8], part), 71), part)
    input_gate = jnp.clip(0.2 + 0.8 * jax.random.uniform(part_splits[6], (TOKEN_LENGTH, HEAD_GROUP), jnp.float32) ** block_scale(part_splits[6], (TOKEN_LENGTH, HEAD_GROUP), ((0, 16),), -0.2, 0.2), 0.2, 1.0)
    regularizer = jnp.clip(jnp.exp(jax.random.uniform(arg_keys[7], (HEAD_GROUP, DK), jnp.float32, math.log(0.5), math.log(4.0))), 0.5, 4.0)
    return {"attn_query": attn_query, "attn_key": attn_key, "attn_value": attn_value, "mesa_query": mesa_query, "mesa_key": mesa_key, "log_decay": log_decay, "input_gate": input_gate, "regularizer": regularizer}


exact_mode = lax.Precision.HIGHEST
masked_score = -1e30


def span_update(states, inputs, ridge_diag):
    gram_start, cross_start = states
    queries, key_rows, value_rows, log_rates, gate_rows = inputs
    q_heads = jnp.transpose(queries, (1, 0, 2))
    k_heads = jnp.transpose(key_rows, (1, 0, 2))
    v_heads = jnp.transpose(value_rows, (1, 0, 2))
    cumulative = jnp.transpose(jnp.cumsum(log_rates, axis=0))
    length = cumulative.shape[1]
    causal = (jnp.arange(length)[:, None] >= jnp.arange(length)[None, :])[None]
    distance = cumulative[:, :, None] - cumulative[:, None, :]
    decay_mix = jnp.where(causal, jnp.exp(jnp.where(causal, distance, 0.0)), 0.0) * jnp.transpose(gate_rows)[:, None, :]
    start_scale = jnp.exp(cumulative)[:, :, None]

    def operator_apply(search):
        carried = start_scale * jnp.einsum('hcd,hed->hce', search, gram_start, precision=exact_mode)
        products = jnp.einsum('hjd,hid->hji', search, k_heads, precision=exact_mode)
        local_part = jnp.einsum('hji,hid->hjd', decay_mix * products, k_heads, precision=exact_mode)
        return carried + local_part + ridge_diag[:, None, :] * search

    iterate = jnp.zeros_like(q_heads)
    remain = q_heads
    search = q_heads
    norm_now = jnp.sum(remain * remain, axis=-1, keepdims=True)
    for sweep_index in range(CG_ITERS):
        image_vec = operator_apply(search)
        step_size = norm_now / (jnp.sum(search * image_vec, axis=-1, keepdims=True) + 1e-6)
        iterate = iterate + step_size * search
        remain = remain - step_size * image_vec
        norm_next = jnp.sum(remain * remain, axis=-1, keepdims=True)
        search = remain + (norm_next / (norm_now + 1e-6)) * search
        norm_now = norm_next
    products = jnp.einsum('hjd,hid->hji', iterate, k_heads, precision=exact_mode)
    mesa_rows = start_scale * jnp.einsum('hje,hde->hjd', iterate, cross_start, precision=exact_mode)
    mesa_rows = mesa_rows + jnp.einsum('hji,hid->hjd', decay_mix * products, v_heads, precision=exact_mode)
    tail_weight = (jnp.exp(cumulative[:, -1:] - cumulative) * jnp.transpose(gate_rows))[:, :, None]
    end_scale = jnp.exp(cumulative[:, -1])[:, None, None]
    gram_end = end_scale * gram_start + jnp.einsum('hid,hie->hde', k_heads * tail_weight, k_heads, precision=exact_mode)
    cross_end = end_scale * cross_start + jnp.einsum('hid,hie->hde', v_heads * tail_weight, k_heads, precision=exact_mode)
    return (gram_end, cross_end), jnp.transpose(mesa_rows, (1, 0, 2))


def mesa_pass(queries, key_rows, value_rows, log_rates, gate_rows, ridge_diag, gram_start, cross_start):
    row_total = queries.shape[0]
    span_count = row_total // SPAN

    def shaped(array_in):
        return array_in.reshape((span_count, SPAN) + array_in.shape[1:])

    def advance(states, inputs):
        return span_update(states, inputs, ridge_diag)

    finished, outputs = lax.scan(advance, (gram_start, cross_start),
                                 (shaped(queries), shaped(key_rows), shaped(value_rows), shaped(log_rates), shaped(gate_rows)))
    return outputs.reshape(row_total, -1)


def reference(attn_query, attn_key, attn_value, mesa_query, mesa_key, log_decay, input_gate, regularizer):
    head_count, head_size = regularizer.shape
    total_rows = attn_query.shape[0]
    block_rows = TOK_DEV
    block_count = total_rows // block_rows
    queries = attn_query.reshape(block_count, block_rows, head_count, head_size)
    padded_keys = jnp.pad(attn_key, ((WINDOW, 0), (0, 0)))
    padded_values = jnp.pad(attn_value, ((WINDOW, 0), (0, 0)))
    scale_factor = head_size ** -0.5

    def attend(inputs):
        block_index, block_queries = inputs
        first_row = (block_index * block_rows).astype(jnp.int32)
        key_rows = lax.dynamic_slice_in_dim(padded_keys, first_row, WINDOW + block_rows, 0).reshape(-1, head_count, head_size)
        value_rows = lax.dynamic_slice_in_dim(padded_values, first_row, WINDOW + block_rows, 0).reshape(-1, head_count, head_size)
        scores = jnp.einsum('qhd,khd->hqk', block_queries.astype(jnp.float32), key_rows.astype(jnp.float32)) * scale_factor
        query_pos = first_row + jnp.arange(block_rows, dtype=jnp.int32)[:, None]
        key_pos = first_row - WINDOW + jnp.arange(WINDOW + block_rows, dtype=jnp.int32)[None, :]
        distance = query_pos - key_pos
        inside = ((distance >= 0) & (distance < WINDOW) & (key_pos >= 0))[None]
        scores = jnp.where(inside, scores, masked_score)
        row_max = jnp.max(scores, axis=-1, keepdims=True)
        weights = jnp.exp(scores - row_max) * inside.astype(jnp.float32)
        rounded = weights.astype(jnp.bfloat16)
        summed = jnp.einsum('hqk,khd->hqd', rounded.astype(jnp.float32), value_rows.astype(jnp.float32))
        normed = summed / jnp.sum(weights, axis=-1, keepdims=True)
        return jnp.transpose(normed, (1, 0, 2)).reshape(block_rows, -1).astype(jnp.bfloat16)

    attention = lax.map(attend, (jnp.arange(block_count, dtype=jnp.int32), queries)).reshape(total_rows, -1)
    shape3 = (total_rows, head_count, head_size)
    gram_zero = jnp.zeros((head_count, head_size, head_size), jnp.float32)
    mesa_out = mesa_pass(mesa_query.astype(jnp.float32).reshape(shape3), mesa_key.astype(jnp.float32).reshape(shape3),
                         attention.astype(jnp.float32).reshape(shape3), log_decay, input_gate, regularizer,
                         gram_zero, gram_zero)
    return attention, mesa_out.astype(jnp.bfloat16)
```

```python
import functools
import math

import jax
import jax.numpy as jnp
from jax import lax
from jax.experimental import pallas as pl
from jax.experimental.pallas import tpu as pltpu
from jax.sharding import PartitionSpec as P

WINDOW = 2048
SPAN = 64
CG_ITERS = 8


exact_mode = lax.Precision.HIGHEST
masked_score = -1e30


def prefix(shard, axis, join, neutral):
    place = lax.axis_index(axis)
    gathered = jax.tree.map(
        lambda a, kind: lax.all_gather(a.astype(kind), axis), shard, (jnp.bfloat16, jnp.bfloat16)
    )
    state = jax.tree.map(lambda a, e: jnp.zeros_like(a) + jnp.asarray(e, a.dtype), shard, neutral)

    def one(lap, state):
        return join(
            state,
            jax.tree.map(
                lambda a, own: lax.dynamic_index_in_dim(a, lap, 0, False).astype(own.dtype),
                gathered,
                shard,
            ),
        )

    return lax.fori_loop(0, place, one, state)


def passed_along(value, axis, steps):
    count = lax.axis_size(axis)
    first, last = (max(0, -steps), min(count, count - steps))
    return lax.ppermute(value, axis, [(source, source + steps) for source in range(first, last)])


def span_update(states, inputs, ridge_diag):
    gram_start, cross_start = states
    queries, key_rows, value_rows, log_rates, gate_rows = inputs
    q_heads = jnp.transpose(queries, (1, 0, 2))
    k_heads = jnp.transpose(key_rows, (1, 0, 2))
    v_heads = jnp.transpose(value_rows, (1, 0, 2))
    cumulative = jnp.transpose(jnp.cumsum(log_rates, axis=0))
    length = cumulative.shape[1]
    causal = (jnp.arange(length)[:, None] >= jnp.arange(length)[None, :])[None]
    distance = cumulative[:, :, None] - cumulative[:, None, :]
    decay_mix = (
        jnp.where(causal, jnp.exp(jnp.where(causal, distance, 0.0)), 0.0)
        * jnp.transpose(gate_rows)[:, None, :]
    )
    start_scale = jnp.exp(cumulative)[:, :, None]
    iterate = jnp.zeros_like(q_heads)
    remain = q_heads
    search = q_heads
    norm_now = jnp.sum(remain * remain, axis=-1, keepdims=True)
    for sweep_index in range(CG_ITERS):
        carried = start_scale * jnp.einsum("hcd,hed->hce", search, gram_start, precision=exact_mode)
        operator_products = jnp.einsum("hjd,hid->hji", search, k_heads, precision=exact_mode)
        local_part = jnp.einsum(
            "hji,hid->hjd", decay_mix * operator_products, k_heads, precision=exact_mode
        )
        image_vec = carried + local_part + ridge_diag[:, None, :] * search
        step_size = norm_now / (jnp.sum(search * image_vec, axis=-1, keepdims=True) + 1e-06)
        iterate = iterate + step_size * search
        remain = remain - step_size * image_vec
        norm_next = jnp.sum(remain * remain, axis=-1, keepdims=True)
        search = remain + norm_next / (norm_now + 1e-06) * search
        norm_now = norm_next
    products = jnp.einsum("hjd,hid->hji", iterate, k_heads, precision=exact_mode)
    mesa_rows = start_scale * jnp.einsum("hje,hde->hjd", iterate, cross_start, precision=exact_mode)
    mesa_rows = mesa_rows + jnp.einsum(
        "hji,hid->hjd", decay_mix * products, v_heads, precision=exact_mode
    )
    tail_weight = (jnp.exp(cumulative[:, -1:] - cumulative) * jnp.transpose(gate_rows))[:, :, None]
    end_scale = jnp.exp(cumulative[:, -1])[:, None, None]
    gram_end = end_scale * gram_start + jnp.einsum(
        "hid,hie->hde", k_heads * tail_weight, k_heads, precision=exact_mode
    )
    cross_end = end_scale * cross_start + jnp.einsum(
        "hid,hie->hde", v_heads * tail_weight, k_heads, precision=exact_mode
    )
    return ((gram_end, cross_end), jnp.transpose(mesa_rows, (1, 0, 2)))


def mesa_pass(
    queries, key_rows, value_rows, log_rates, gate_rows, ridge_diag, gram_start, cross_start
):
    row_total = queries.shape[0]
    span_count = row_total // SPAN

    def shaped(array_in):
        return array_in.reshape((span_count, SPAN) + array_in.shape[1:])

    def advance(states, inputs):
        return span_update(states, inputs, ridge_diag)

    finished, outputs = lax.scan(
        advance,
        (gram_start, cross_start),
        (
            shaped(queries),
            shaped(key_rows),
            shaped(value_rows),
            shaped(log_rates),
            shaped(gate_rows),
        ),
    )
    return outputs.reshape(row_total, -1)


def fold_block(state_now, queries, key_value, query_first, key_first):
    running_max, running_sum, weighted = state_now
    row_count, head_count, head_size = queries.shape
    key_rows = key_value[0].reshape(-1, head_count, head_size)
    value_rows = key_value[1].reshape(-1, head_count, head_size)
    scores = jnp.einsum(
        "qhd,khd->hqk", queries, key_rows, preferred_element_type=jnp.float32
    ) * head_size ** (-0.5)
    query_pos = query_first + jnp.arange(row_count, dtype=jnp.int32)[:, None]
    key_pos = key_first + jnp.arange(key_rows.shape[0], dtype=jnp.int32)[None, :]
    distance = query_pos - key_pos
    inside = ((distance >= 0) & (distance < WINDOW) & (key_pos >= 0))[None]
    scores = jnp.where(inside, scores, masked_score)
    new_max = jnp.maximum(running_max, jnp.max(scores, axis=-1))
    weights = jnp.exp(scores - new_max[:, :, None]) * inside.astype(jnp.float32)
    rescale = jnp.exp(running_max - new_max)
    running_sum = running_sum * rescale + jnp.sum(weights, axis=-1)
    weighted = weighted * rescale[:, :, None] + jnp.einsum(
        "hqk,khd->hqd", weights.astype(jnp.bfloat16), value_rows, preferred_element_type=jnp.float32
    )
    return (new_max, running_sum, weighted)


def combine_pair(earlier, later):
    return (earlier[0] + later[0], jnp.exp(later[0])[:, None, None] * earlier[1] + later[1])


def split_cat(value, axis):
    high = value.astype(jnp.bfloat16)
    low = (value - high.astype(jnp.float32)).astype(jnp.bfloat16)
    return jnp.concatenate([high, low], axis=axis)


def dot_nn(a, b):
    return lax.dot_general(a, b, (((1,), (0,)), ((), ())), preferred_element_type=jnp.float32)


def dot_nt(a, b):
    return lax.dot_general(a, b, (((1,), (1,)), ((), ())), preferred_element_type=jnp.float32)


def attend_kernel(qkv_ref, out_ref, *, rows, reach):
    i = pl.program_id(0)
    size = qkv_ref.shape[-1]
    factor = size ** (-0.5) * math.log2(math.e)
    col = lax.broadcasted_iota(jnp.int32, (rows, rows), 1)
    row = lax.broadcasted_iota(jnp.int32, (rows, rows), 0)

    def run(first, count, full):
        q = qkv_ref[i, pl.ds(0, rows), :]
        scores = []
        for c in range(count):
            s = dot_nt(q, qkv_ref[first + c, pl.ds(rows, rows), :])
            if full:
                if c == 0:
                    s = jnp.where(col > row, s, masked_score)
                elif c == count - 1:
                    s = jnp.where(col <= row, s, masked_score)
            else:
                s = jnp.where(col - row <= (i - c) * rows, s, masked_score)
            scores.append(s)
        top = jnp.max(functools.reduce(jnp.maximum, scores), axis=-1, keepdims=True)
        total = None
        acc = None
        for c in range(count):
            w = jnp.exp2((scores[c] - top) * factor)
            part = dot_nn(w.astype(jnp.bfloat16), qkv_ref[first + c, pl.ds(2 * rows, rows), :])
            total = w if total is None else total + w
            acc = part if acc is None else acc + part
        total = jnp.sum(total, axis=-1, keepdims=True)
        out_ref[0] = (acc / total).astype(out_ref.dtype)

    bounds = sorted({max(1, reach // 2), reach})
    low = 0
    for bound in bounds:
        pl.when((i >= low) & (i < bound))(functools.partial(run, 0, bound, False))
        low = bound
    pl.when(i >= reach)(lambda: run(i - reach, reach + 1, True))


def attend(qkv, rows, reach):
    slabs, _, size = qkv.shape
    return pl.pallas_call(
        functools.partial(attend_kernel, rows=rows, reach=reach),
        grid=(slabs,),
        in_specs=[pl.BlockSpec(qkv.shape, lambda i: (0, 0, 0))],
        out_specs=pl.BlockSpec((1, rows, size), lambda i: (i, 0, 0)),
        out_shape=jax.ShapeDtypeStruct((slabs, rows, size), jnp.bfloat16),
        name="attend",
    )(qkv)


def states_kernel(k_ref, x_ref, w_ref, out_ref):
    slabs, rows, size = k_ref.shape
    state = jnp.zeros((size, size), jnp.float32)
    for j in range(slabs):
        out_ref[j] = state.astype(out_ref.dtype)
        if j == slabs - 1:
            break
        weighted = jnp.transpose(k_ref[j].astype(jnp.float32)) * w_ref[j, 0:1, :]
        x = x_ref[j]
        fresh = dot_nn(split_cat(weighted, 1), jnp.concatenate([x, x], axis=0))
        state = w_ref[j, 1:2, :size] * state + fresh


def states(keys, others, weights):
    slabs, rows, size = keys.shape
    return pl.pallas_call(
        states_kernel,
        out_shape=jax.ShapeDtypeStruct((slabs, size, size), jnp.bfloat16),
        name="states",
    )(keys, others, weights)


def solve_kernel(q_ref, k_ref, rate_ref, gate_ref, ridge_ref, gram_ref, x_ref, p_ref):
    rows = q_ref.shape[0]
    heads, size = ridge_ref.shape[1:]
    causal = lax.broadcasted_iota(jnp.int32, (rows, rows), 0) >= lax.broadcasted_iota(
        jnp.int32, (rows, rows), 1
    )
    held = []
    for h in range(heads):
        cols = slice(h * size, (h + 1) * size)
        key = k_ref[:, cols]
        by_col = jnp.broadcast_to(rate_ref[0, h : h + 1, :], (rows, rows))
        by_row = jnp.transpose(by_col)
        mix = (
            jnp.where(causal, jnp.exp(jnp.where(causal, by_row - by_col, 0.0)), 0.0)
            * gate_ref[0, h : h + 1, :]
        )
        gram = gram_ref[h]
        query = q_ref[:, cols].astype(jnp.float32)
        held.append(
            dict(
                wide=jnp.concatenate([key, key], axis=1),
                tall=jnp.concatenate([key, key], axis=0),
                gram=jnp.concatenate([gram, gram], axis=0),
                mix=mix,
                scale=jnp.exp(by_row[:, :size]),
                ridge=ridge_ref[0, h : h + 1, :],
                x=jnp.zeros_like(query),
                r=query,
                p=query,
                rr=jnp.sum(query * query, axis=-1, keepdims=True),
            )
        )
    for _ in range(CG_ITERS):
        for s in held:
            p = s["p"]
            parts = split_cat(p, 1)
            products = split_cat(s["mix"] * dot_nt(parts, s["wide"]), 1)
            image = (
                s["scale"] * dot_nn(parts, s["gram"]) + dot_nn(products, s["tall"]) + s["ridge"] * p
            )
            alpha = s["rr"] / (jnp.sum(p * image, axis=-1, keepdims=True) + 1e-6)
            s["x"] = s["x"] + alpha * p
            s["r"] = s["r"] - alpha * image
            new = jnp.sum(s["r"] * s["r"], axis=-1, keepdims=True)
            s["p"] = s["r"] + (new / (s["rr"] + 1e-6)) * p
            s["rr"] = new
    for h, s in enumerate(held):
        x_ref[h] = (s["scale"] * s["x"]).astype(x_ref.dtype)
        p_ref[h] = (s["mix"] * dot_nt(split_cat(s["x"], 1), s["wide"])).astype(p_ref.dtype)


def solve(queries, keys, rates, gates, ridge, gram, group):
    rows = queries.shape[0]
    heads, size = ridge.shape
    steps = heads // group

    def packed(a):
        return a.reshape(steps, group, a.shape[-1])

    def small(width):
        return pl.BlockSpec((1, group, width), lambda i: (i, 0, 0))

    wide = pl.BlockSpec((rows, group * size), lambda i: (0, i))
    return pl.pallas_call(
        solve_kernel,
        grid=(steps,),
        in_specs=[
            wide,
            wide,
            small(rows),
            small(rows),
            small(size),
            pl.BlockSpec((group, size, size), lambda i: (i, 0, 0)),
        ],
        out_specs=[
            pl.BlockSpec((group, rows, size), lambda i: (i, 0, 0)),
            pl.BlockSpec((group, rows, rows), lambda i: (i, 0, 0)),
        ],
        out_shape=[
            jax.ShapeDtypeStruct((heads, rows, size), jnp.bfloat16),
            jax.ShapeDtypeStruct((heads, rows, rows), jnp.bfloat16),
        ],
        name="solve",
    )(queries, keys, packed(rates), packed(gates), packed(ridge), gram)


def finish_kernel(x_ref, p_ref, v_ref, cross_ref, att_ref, out_ref):
    heads, rows, size = x_ref.shape
    for h in range(heads):
        cols = slice(h * size, (h + 1) * size)
        value = v_ref[h]
        att_ref[:, cols] = value
        out_ref[:, cols] = (dot_nn(x_ref[h], cross_ref[h]) + dot_nn(p_ref[h], value)).astype(
            out_ref.dtype
        )


def finish(x, products, values, cross, group):
    heads, rows, size = x.shape

    def spec(a):
        return pl.BlockSpec((group,) + a.shape[1:], lambda i: (i, 0, 0))

    flat = pl.BlockSpec((rows, group * size), lambda i: (0, i))
    shape = jax.ShapeDtypeStruct((rows, heads * size), jnp.bfloat16)
    return pl.pallas_call(
        finish_kernel,
        grid=(heads // group,),
        in_specs=[spec(x), spec(products), spec(values), spec(cross)],
        out_specs=[flat, flat],
        out_shape=[shape, shape],
        name="finish",
    )(x, products, values, cross)


def exchange(value):
    return lax.all_to_all(value, "seq", 0, 0, tiled=True)


def by_head(value, heads):
    rows = value.shape[0]
    return jnp.transpose(value.reshape(rows, heads, -1), (1, 0, 2))


def head_body(
    attn_query, attn_key, attn_value, mesa_query, mesa_key, log_decay, input_gate, regularizer
):
    rows = attn_query.shape[0]
    heads, size = regularizer.shape
    lower = jnp.tril(jnp.ones((rows, rows), jnp.float32))
    rates = jnp.einsum("th,st->hs", log_decay, lower, precision=exact_mode)
    gates = jnp.transpose(input_gate)
    last = rates[:, -1:]
    weights = jnp.stack(
        [jnp.exp(last - rates) * gates, jnp.broadcast_to(jnp.exp(last), rates.shape)], axis=1
    )
    qkv = exchange(
        jnp.concatenate([by_head(a, heads) for a in (attn_query, attn_key, attn_value)], axis=1)
    )
    weights = exchange(weights)
    keys = exchange(by_head(mesa_key, heads))
    gram = exchange(states(keys, keys, weights))
    values = attend(qkv, rows, WINDOW // rows)
    local_values = exchange(values)
    cross = exchange(states(keys, values, weights))
    group = 2 if heads % 2 == 0 else 1
    x, products = solve(mesa_query, mesa_key, rates, gates, regularizer, gram, group)
    return tuple(finish(x, products, local_values, cross, group))


def body(
    attn_query, attn_key, attn_value, mesa_query, mesa_key, log_decay, input_gate, regularizer
):
    row_count = attn_query.shape[0]
    head_count, head_size = regularizer.shape
    shape3 = (row_count, head_count, head_size)
    slab_first = lax.axis_index("seq") * row_count
    keys_float = mesa_key.astype(jnp.float32).reshape(shape3)
    slab_log = jnp.sum(log_decay, axis=0)
    tail_log = slab_log[None, :] - jnp.cumsum(log_decay, axis=0)
    weight_rows = (jnp.exp(tail_log) * input_gate)[:, :, None]
    gram_local = jnp.einsum(
        "lhd,lhe->hde", keys_float * weight_rows, keys_float, precision=exact_mode
    )
    zero_log = jnp.zeros_like(slab_log)
    zero_state = jnp.zeros_like(gram_local)
    gram_prefix = prefix((slab_log, gram_local), "seq", combine_pair, (zero_log, zero_state))[1]
    queries = attn_query.reshape(shape3)
    key_value = jnp.stack([attn_key, attn_value])
    state_now = (
        jnp.full((head_count, row_count), masked_score, jnp.float32),
        jnp.zeros((head_count, row_count), jnp.float32),
        jnp.zeros((head_count, row_count, head_size), jnp.float32),
    )
    state_now = fold_block(state_now, queries, key_value, slab_first, slab_first)
    reach = -(-WINDOW // row_count)
    moving = key_value
    for hop_index in range(1, reach + 1):
        moving = passed_along(moving, "seq", 1)
        state_now = fold_block(
            state_now, queries, moving, slab_first, slab_first - hop_index * row_count
        )
    normed = state_now[2] / state_now[1][:, :, None]
    attention = jnp.transpose(normed, (1, 0, 2)).reshape(row_count, -1).astype(jnp.bfloat16)
    values_float = attention.astype(jnp.float32).reshape(shape3)
    cross_local = jnp.einsum(
        "lhd,lhe->hde", values_float * weight_rows, keys_float, precision=exact_mode
    )
    cross_prefix = prefix((slab_log, cross_local), "seq", combine_pair, (zero_log, zero_state))[1]
    mesa_out = mesa_pass(
        mesa_query.astype(jnp.float32).reshape(shape3),
        keys_float,
        values_float,
        log_decay,
        input_gate,
        regularizer,
        gram_prefix,
        cross_prefix,
    )
    return (attention, mesa_out.astype(jnp.bfloat16))


def solution(mesh):
    def chosen(*arrays):
        rows = arrays[0].shape[0]
        heads, size = arrays[-1].shape
        fits = WINDOW % rows == 0 and rows % 128 == 0 and size == 128
        if heads == mesh.shape["seq"] and fits:
            return head_body(*arrays)
        return body(*arrays)

    return jax.shard_map(
        chosen,
        mesh=mesh,
        in_specs=(
            P(("groups", "seq"), None),
            P(("groups", "seq"), None),
            P(("groups", "seq"), None),
            P(("groups", "seq"), None),
            P(("groups", "seq"), None),
            P(("groups", "seq"), None),
            P(("groups", "seq"), None),
            P(),
        ),
        out_specs=(P(("groups", "seq"), None), P(("groups", "seq"), None)),
        check_vma=False,
    )
```

```python
import functools
import math

import jax
import jax.numpy as jnp
from jax import lax
from jax.experimental import pallas as pl
from jax.experimental.pallas import tpu as pltpu
from jax.sharding import PartitionSpec as P

WINDOW = 2048
SPAN = 64
CG_ITERS = 8


exact_mode = lax.Precision.HIGHEST
masked_score = -1e30


def prefix(shard, axis, join, neutral):
    place = lax.axis_index(axis)
    gathered = jax.tree.map(
        lambda a, kind: lax.all_gather(a.astype(kind), axis), shard, (jnp.bfloat16, jnp.bfloat16)
    )
    state = jax.tree.map(lambda a, e: jnp.zeros_like(a) + jnp.asarray(e, a.dtype), shard, neutral)

    def one(lap, state):
        return join(
            state,
            jax.tree.map(
                lambda a, own: lax.dynamic_index_in_dim(a, lap, 0, False).astype(own.dtype),
                gathered,
                shard,
            ),
        )

    return lax.fori_loop(0, place, one, state)


def passed_along(value, axis, steps):
    count = lax.axis_size(axis)
    first, last = (max(0, -steps), min(count, count - steps))
    return lax.ppermute(value, axis, [(source, source + steps) for source in range(first, last)])


def span_update(states, inputs, ridge_diag):
    gram_start, cross_start = states
    queries, key_rows, value_rows, log_rates, gate_rows = inputs
    q_heads = jnp.transpose(queries, (1, 0, 2))
    k_heads = jnp.transpose(key_rows, (1, 0, 2))
    v_heads = jnp.transpose(value_rows, (1, 0, 2))
    cumulative = jnp.transpose(jnp.cumsum(log_rates, axis=0))
    length = cumulative.shape[1]
    causal = (jnp.arange(length)[:, None] >= jnp.arange(length)[None, :])[None]
    distance = cumulative[:, :, None] - cumulative[:, None, :]
    decay_mix = (
        jnp.where(causal, jnp.exp(jnp.where(causal, distance, 0.0)), 0.0)
        * jnp.transpose(gate_rows)[:, None, :]
    )
    start_scale = jnp.exp(cumulative)[:, :, None]
    iterate = jnp.zeros_like(q_heads)
    remain = q_heads
    search = q_heads
    norm_now = jnp.sum(remain * remain, axis=-1, keepdims=True)
    for sweep_index in range(CG_ITERS):
        carried = start_scale * jnp.einsum("hcd,hed->hce", search, gram_start, precision=exact_mode)
        operator_products = jnp.einsum("hjd,hid->hji", search, k_heads, precision=exact_mode)
        local_part = jnp.einsum(
            "hji,hid->hjd", decay_mix * operator_products, k_heads, precision=exact_mode
        )
        image_vec = carried + local_part + ridge_diag[:, None, :] * search
        step_size = norm_now / (jnp.sum(search * image_vec, axis=-1, keepdims=True) + 1e-06)
        iterate = iterate + step_size * search
        remain = remain - step_size * image_vec
        norm_next = jnp.sum(remain * remain, axis=-1, keepdims=True)
        search = remain + norm_next / (norm_now + 1e-06) * search
        norm_now = norm_next
    products = jnp.einsum("hjd,hid->hji", iterate, k_heads, precision=exact_mode)
    mesa_rows = start_scale * jnp.einsum("hje,hde->hjd", iterate, cross_start, precision=exact_mode)
    mesa_rows = mesa_rows + jnp.einsum(
        "hji,hid->hjd", decay_mix * products, v_heads, precision=exact_mode
    )
    tail_weight = (jnp.exp(cumulative[:, -1:] - cumulative) * jnp.transpose(gate_rows))[:, :, None]
    end_scale = jnp.exp(cumulative[:, -1])[:, None, None]
    gram_end = end_scale * gram_start + jnp.einsum(
        "hid,hie->hde", k_heads * tail_weight, k_heads, precision=exact_mode
    )
    cross_end = end_scale * cross_start + jnp.einsum(
        "hid,hie->hde", v_heads * tail_weight, k_heads, precision=exact_mode
    )
    return ((gram_end, cross_end), jnp.transpose(mesa_rows, (1, 0, 2)))


def mesa_pass(
    queries, key_rows, value_rows, log_rates, gate_rows, ridge_diag, gram_start, cross_start
):
    row_total = queries.shape[0]
    span_count = row_total // SPAN

    def shaped(array_in):
        return array_in.reshape((span_count, SPAN) + array_in.shape[1:])

    def advance(states, inputs):
        return span_update(states, inputs, ridge_diag)

    finished, outputs = lax.scan(
        advance,
        (gram_start, cross_start),
        (
            shaped(queries),
            shaped(key_rows),
            shaped(value_rows),
            shaped(log_rates),
            shaped(gate_rows),
        ),
    )
    return outputs.reshape(row_total, -1)


def fold_block(state_now, queries, key_value, query_first, key_first):
    running_max, running_sum, weighted = state_now
    row_count, head_count, head_size = queries.shape
    key_rows = key_value[0].reshape(-1, head_count, head_size)
    value_rows = key_value[1].reshape(-1, head_count, head_size)
    scores = jnp.einsum(
        "qhd,khd->hqk", queries, key_rows, preferred_element_type=jnp.float32
    ) * head_size ** (-0.5)
    query_pos = query_first + jnp.arange(row_count, dtype=jnp.int32)[:, None]
    key_pos = key_first + jnp.arange(key_rows.shape[0], dtype=jnp.int32)[None, :]
    distance = query_pos - key_pos
    inside = ((distance >= 0) & (distance < WINDOW) & (key_pos >= 0))[None]
    scores = jnp.where(inside, scores, masked_score)
    new_max = jnp.maximum(running_max, jnp.max(scores, axis=-1))
    weights = jnp.exp(scores - new_max[:, :, None]) * inside.astype(jnp.float32)
    rescale = jnp.exp(running_max - new_max)
    running_sum = running_sum * rescale + jnp.sum(weights, axis=-1)
    weighted = weighted * rescale[:, :, None] + jnp.einsum(
        "hqk,khd->hqd", weights.astype(jnp.bfloat16), value_rows, preferred_element_type=jnp.float32
    )
    return (new_max, running_sum, weighted)


def combine_pair(earlier, later):
    return (earlier[0] + later[0], jnp.exp(later[0])[:, None, None] * earlier[1] + later[1])


def split_cat(value, axis):
    high = value.astype(jnp.bfloat16)
    low = (value - high.astype(jnp.float32)).astype(jnp.bfloat16)
    return jnp.concatenate([high, low], axis=axis)


def dot_nn(a, b):
    return lax.dot_general(a, b, (((1,), (0,)), ((), ())), preferred_element_type=jnp.float32)


def dot_nt(a, b):
    return lax.dot_general(a, b, (((1,), (1,)), ((), ())), preferred_element_type=jnp.float32)


def fresh_state(packed, others):
    rows = others.shape[0]
    keys = packed[:rows].astype(jnp.float32)
    extra = packed[rows:].astype(jnp.float32)
    count = rows // packed.shape[1]
    weights = extra[:count] + extra[count : 2 * count]
    weights = jnp.concatenate([weights[c : c + 1] for c in range(count)], axis=1)
    decay = extra[2 * count : 2 * count + 1] + extra[2 * count + 1 : 2 * count + 2]
    weighted = split_cat(jnp.transpose(keys) * weights, 1)
    return decay, dot_nn(weighted, jnp.concatenate([others, others], axis=0))


def pack_keys_kernel(k_ref, rate_ref, gate_ref, out_ref, total_ref, gate_out_ref):
    heads, height, size = out_ref.shape
    rows = k_ref.shape[0]
    count = rows // size
    at = lax.broadcasted_iota(jnp.int32, (rows, rows), 0)
    lower = (at >= lax.broadcasted_iota(jnp.int32, (rows, rows), 1)).astype(jnp.float32)
    totals = jnp.transpose(
        lax.dot_general(
            lower,
            rate_ref[...],
            (((1,), (0,)), ((), ())),
            precision=exact_mode,
            preferred_element_type=jnp.float32,
        )
    )
    gates = jnp.transpose(gate_ref[...])
    total_ref[...] = totals
    gate_out_ref[...] = gates
    last = totals[:, rows - 1 :]
    weights = jnp.exp(last - totals) * gates
    decays = jnp.broadcast_to(jnp.exp(last), (heads, size))
    place = lax.broadcasted_iota(jnp.int32, (height - rows, size), 0)
    for h in range(heads):
        pieces = [weights[h : h + 1, c * size : (c + 1) * size] for c in range(count)]
        high = [p.astype(jnp.bfloat16).astype(jnp.float32) for p in pieces]
        decay = decays[h : h + 1]
        decay_high = decay.astype(jnp.bfloat16).astype(jnp.float32)
        lines = high + [p - q for p, q in zip(pieces, high)] + [decay_high, decay - decay_high]
        tile = jnp.zeros((height - rows, size), jnp.float32)
        for n, line in enumerate(lines):
            tile = jnp.where(place == n, line, tile)
        out_ref[h, :rows, :] = k_ref[:, h * size : (h + 1) * size]
        out_ref[h, rows:, :] = tile.astype(jnp.bfloat16)


def pack_keys(keys, rates, gates, size):
    rows, features = keys.shape
    heads = features // size
    spare = -(-(2 * (rows // size) + 2) // 16) * 16
    small = jax.ShapeDtypeStruct((heads, rows), jnp.float32)
    return pl.pallas_call(
        pack_keys_kernel,
        out_shape=[
            jax.ShapeDtypeStruct((heads, rows + spare, size), jnp.bfloat16),
            small,
            small,
        ],
        name="pack_keys",
    )(keys, rates, gates)


def attend_kernel(qkv_ref, key_ref, out_ref, state_ref, *, rows, reach):
    i = pl.program_id(0)
    size = qkv_ref.shape[-1]
    factor = size ** (-0.5) * math.log2(math.e)
    col = lax.broadcasted_iota(jnp.int32, (rows, rows), 1)
    row = lax.broadcasted_iota(jnp.int32, (rows, rows), 0)

    def run(first, count, full):
        q = qkv_ref[i, pl.ds(0, rows), :]
        scores = []
        for c in range(count):
            s = dot_nt(q, qkv_ref[first + c, pl.ds(rows, rows), :])
            if full:
                if c == 0:
                    s = jnp.where(col > row, s, masked_score)
                elif c == count - 1:
                    s = jnp.where(col <= row, s, masked_score)
            else:
                s = jnp.where(col - row <= (i - c) * rows, s, masked_score)
            scores.append(s)
        top = jnp.max(functools.reduce(jnp.maximum, scores), axis=-1, keepdims=True)
        total = None
        acc = None
        for c in range(count):
            w = jnp.exp2((scores[c] - top) * factor)
            part = dot_nn(w.astype(jnp.bfloat16), qkv_ref[first + c, pl.ds(2 * rows, rows), :])
            total = w if total is None else total + w
            acc = part if acc is None else acc + part
        total = jnp.sum(total, axis=-1, keepdims=True)
        value = (acc / total).astype(out_ref.dtype)
        out_ref[0, :rows, :] = value
        decay, fresh = fresh_state(key_ref[i], value)
        state = state_ref[...]
        out_ref[0, rows:, :] = state.astype(out_ref.dtype)
        state_ref[...] = decay * state + fresh

    @pl.when(i == 0)
    def _():
        state_ref[...] = jnp.zeros_like(state_ref)

    bounds = sorted({max(1, reach * n // 4) for n in range(1, 5)})
    low = 0
    for bound in bounds:
        pl.when((i >= low) & (i < bound))(functools.partial(run, 0, bound, False))
        low = bound
    pl.when(i >= reach)(lambda: run(i - reach, reach + 1, True))


def attend(qkv, keys, rows, reach):
    slabs, _, size = qkv.shape
    return pl.pallas_call(
        functools.partial(attend_kernel, rows=rows, reach=reach),
        grid=(slabs,),
        in_specs=[
            pl.BlockSpec(qkv.shape, lambda i: (0, 0, 0)),
            pl.BlockSpec(keys.shape, lambda i: (0, 0, 0)),
        ],
        out_specs=pl.BlockSpec((1, rows + size, size), lambda i: (i, 0, 0)),
        out_shape=jax.ShapeDtypeStruct((slabs, rows + size, size), jnp.bfloat16),
        scratch_shapes=[pltpu.VMEM((size, size), jnp.float32)],
        name="attend",
    )(qkv, keys)


def grams_kernel(k_ref, out_ref, *, rows):
    slabs, _, size = k_ref.shape
    state = jnp.zeros((size, size), jnp.float32)
    for j in range(slabs):
        out_ref[j] = state.astype(out_ref.dtype)
        if j < slabs - 1:
            decay, fresh = fresh_state(k_ref[j], k_ref[j, :rows, :])
            state = decay * state + fresh


def grams(keys, rows):
    slabs, _, size = keys.shape
    return pl.pallas_call(
        functools.partial(grams_kernel, rows=rows),
        out_shape=jax.ShapeDtypeStruct((slabs, size, size), jnp.bfloat16),
        name="grams",
    )(keys)


def solve_kernel(q_ref, k_ref, rate_ref, gate_ref, ridge_ref, gram_ref, x_ref, p_ref):
    rows = q_ref.shape[0]
    heads, size = ridge_ref.shape[1:]
    causal = lax.broadcasted_iota(jnp.int32, (rows, rows), 0) >= lax.broadcasted_iota(
        jnp.int32, (rows, rows), 1
    )
    held = []
    for h in range(heads):
        cols = slice(h * size, (h + 1) * size)
        key = k_ref[:, cols]
        by_col = jnp.broadcast_to(rate_ref[0, h : h + 1, :], (rows, rows))
        by_row = jnp.transpose(by_col)
        mix = (
            jnp.where(causal, jnp.exp(jnp.where(causal, by_row - by_col, 0.0)), 0.0)
            * gate_ref[0, h : h + 1, :]
        )
        gram = gram_ref[h]
        query = q_ref[:, cols].astype(jnp.float32)
        held.append(
            dict(
                wide=jnp.concatenate([key, key], axis=1),
                tall=jnp.concatenate([key, key], axis=0),
                gram=jnp.concatenate([gram, gram], axis=0),
                mix=mix,
                scale=jnp.exp(by_row[:, :size]),
                ridge=ridge_ref[0, h : h + 1, :],
                x=jnp.zeros_like(query),
                r=query,
                p=query,
                rr=jnp.sum(query * query, axis=-1, keepdims=True),
            )
        )
    for _ in range(CG_ITERS):
        for s in held:
            p = s["p"]
            parts = split_cat(p, 1)
            products = split_cat(s["mix"] * dot_nt(parts, s["wide"]), 1)
            image = (
                s["scale"] * dot_nn(parts, s["gram"]) + dot_nn(products, s["tall"]) + s["ridge"] * p
            )
            alpha = s["rr"] / (jnp.sum(p * image, axis=-1, keepdims=True) + 1e-6)
            s["x"] = s["x"] + alpha * p
            s["r"] = s["r"] - alpha * image
            new = jnp.sum(s["r"] * s["r"], axis=-1, keepdims=True)
            s["p"] = s["r"] + (new / (s["rr"] + 1e-6)) * p
            s["rr"] = new
    for h, s in enumerate(held):
        x_ref[h] = (s["scale"] * s["x"]).astype(x_ref.dtype)
        p_ref[h] = (s["mix"] * dot_nt(split_cat(s["x"], 1), s["wide"])).astype(p_ref.dtype)


def solve(queries, keys, rates, gates, ridge, gram, group):
    rows = queries.shape[0]
    heads, size = ridge.shape
    steps = heads // group

    def packed(a):
        return a.reshape(steps, group, a.shape[-1])

    def small(width):
        return pl.BlockSpec((1, group, width), lambda i: (i, 0, 0))

    wide = pl.BlockSpec((rows, group * size), lambda i: (0, i))
    return pl.pallas_call(
        solve_kernel,
        grid=(steps,),
        in_specs=[
            wide,
            wide,
            small(rows),
            small(rows),
            small(size),
            pl.BlockSpec((group, size, size), lambda i: (i, 0, 0)),
        ],
        out_specs=[
            pl.BlockSpec((group, rows, size), lambda i: (i, 0, 0)),
            pl.BlockSpec((group, rows, rows), lambda i: (i, 0, 0)),
        ],
        out_shape=[
            jax.ShapeDtypeStruct((heads, rows, size), jnp.bfloat16),
            jax.ShapeDtypeStruct((heads, rows, rows), jnp.bfloat16),
        ],
        name="solve",
    )(queries, keys, packed(rates), packed(gates), packed(ridge), gram)


def finish_kernel(x_ref, p_ref, back_ref, att_ref, out_ref):
    heads, rows, size = x_ref.shape
    for h in range(heads):
        cols = slice(h * size, (h + 1) * size)
        value = back_ref[h, :rows, :]
        att_ref[:, cols] = value
        out_ref[:, cols] = (dot_nn(x_ref[h], back_ref[h, rows:, :]) + dot_nn(p_ref[h], value)).astype(
            out_ref.dtype
        )


def finish(x, products, back, group):
    heads, rows, size = x.shape

    def spec(a):
        return pl.BlockSpec((group,) + a.shape[1:], lambda i: (i, 0, 0))

    flat = pl.BlockSpec((rows, group * size), lambda i: (0, i))
    shape = jax.ShapeDtypeStruct((rows, heads * size), jnp.bfloat16)
    return pl.pallas_call(
        finish_kernel,
        grid=(heads // group,),
        in_specs=[spec(x), spec(products), spec(back)],
        out_specs=[flat, flat],
        out_shape=[shape, shape],
        name="finish",
    )(x, products, back)


def exchange(value):
    return lax.all_to_all(value, "seq", 0, 0, tiled=True)


def by_head(value, heads):
    rows = value.shape[0]
    return jnp.transpose(value.reshape(rows, heads, -1), (1, 0, 2))


def head_body(
    attn_query, attn_key, attn_value, mesa_query, mesa_key, log_decay, input_gate, regularizer
):
    rows = attn_query.shape[0]
    heads, size = regularizer.shape
    packed, rates, gates = pack_keys(mesa_key, log_decay, input_gate, size)
    keys = exchange(packed)
    qkv = exchange(
        jnp.concatenate([by_head(a, heads) for a in (attn_query, attn_key, attn_value)], axis=1)
    )
    gram = exchange(grams(keys, rows))
    back = exchange(attend(qkv, keys, rows, WINDOW // rows))
    group = 2 if heads % 2 == 0 else 1
    x, products = solve(mesa_query, mesa_key, rates, gates, regularizer, gram, group)
    return tuple(finish(x, products, back, group))


def body(
    attn_query, attn_key, attn_value, mesa_query, mesa_key, log_decay, input_gate, regularizer
):
    row_count = attn_query.shape[0]
    head_count, head_size = regularizer.shape
    shape3 = (row_count, head_count, head_size)
    slab_first = lax.axis_index("seq") * row_count
    keys_float = mesa_key.astype(jnp.float32).reshape(shape3)
    slab_log = jnp.sum(log_decay, axis=0)
    tail_log = slab_log[None, :] - jnp.cumsum(log_decay, axis=0)
    weight_rows = (jnp.exp(tail_log) * input_gate)[:, :, None]
    gram_local = jnp.einsum(
        "lhd,lhe->hde", keys_float * weight_rows, keys_float, precision=exact_mode
    )
    zero_log = jnp.zeros_like(slab_log)
    zero_state = jnp.zeros_like(gram_local)
    gram_prefix = prefix((slab_log, gram_local), "seq", combine_pair, (zero_log, zero_state))[1]
    queries = attn_query.reshape(shape3)
    key_value = jnp.stack([attn_key, attn_value])
    state_now = (
        jnp.full((head_count, row_count), masked_score, jnp.float32),
        jnp.zeros((head_count, row_count), jnp.float32),
        jnp.zeros((head_count, row_count, head_size), jnp.float32),
    )
    state_now = fold_block(state_now, queries, key_value, slab_first, slab_first)
    reach = -(-WINDOW // row_count)
    moving = key_value
    for hop_index in range(1, reach + 1):
        moving = passed_along(moving, "seq", 1)
        state_now = fold_block(
            state_now, queries, moving, slab_first, slab_first - hop_index * row_count
        )
    normed = state_now[2] / state_now[1][:, :, None]
    attention = jnp.transpose(normed, (1, 0, 2)).reshape(row_count, -1).astype(jnp.bfloat16)
    values_float = attention.astype(jnp.float32).reshape(shape3)
    cross_local = jnp.einsum(
        "lhd,lhe->hde", values_float * weight_rows, keys_float, precision=exact_mode
    )
    cross_prefix = prefix((slab_log, cross_local), "seq", combine_pair, (zero_log, zero_state))[1]
    mesa_out = mesa_pass(
        mesa_query.astype(jnp.float32).reshape(shape3),
        keys_float,
        values_float,
        log_decay,
        input_gate,
        regularizer,
        gram_prefix,
        cross_prefix,
    )
    return (attention, mesa_out.astype(jnp.bfloat16))


def solution(mesh):
    def chosen(*arrays):
        rows = arrays[0].shape[0]
        heads, size = arrays[-1].shape
        fits = WINDOW % rows == 0 and rows % 128 == 0 and size == 128
        if heads == mesh.shape["seq"] and fits:
            return head_body(*arrays)
        return body(*arrays)

    return jax.shard_map(
        chosen,
        mesh=mesh,
        in_specs=(
            P(("groups", "seq"), None),
            P(("groups", "seq"), None),
            P(("groups", "seq"), None),
            P(("groups", "seq"), None),
            P(("groups", "seq"), None),
            P(("groups", "seq"), None),
            P(("groups", "seq"), None),
            P(),
        ),
        out_specs=(P(("groups", "seq"), None), P(("groups", "seq"), None)),
        check_vma=False,
    )
```

```python
import functools
import math

import jax
import jax.numpy as jnp
from jax import lax
from jax.experimental import pallas as pl
from jax.experimental.pallas import tpu as pltpu
from jax.sharding import PartitionSpec as P

WINDOW = 2048
SPAN = 64
CG_ITERS = 8


exact_mode = lax.Precision.HIGHEST
masked_score = -1e30


def prefix(shard, axis, join, neutral):
    place = lax.axis_index(axis)
    gathered = jax.tree.map(
        lambda a, kind: lax.all_gather(a.astype(kind), axis), shard, (jnp.bfloat16, jnp.bfloat16)
    )
    state = jax.tree.map(lambda a, e: jnp.zeros_like(a) + jnp.asarray(e, a.dtype), shard, neutral)

    def one(lap, state):
        return join(
            state,
            jax.tree.map(
                lambda a, own: lax.dynamic_index_in_dim(a, lap, 0, False).astype(own.dtype),
                gathered,
                shard,
            ),
        )

    return lax.fori_loop(0, place, one, state)


def passed_along(value, axis, steps):
    count = lax.axis_size(axis)
    first, last = (max(0, -steps), min(count, count - steps))
    return lax.ppermute(value, axis, [(source, source + steps) for source in range(first, last)])


def span_update(states, inputs, ridge_diag):
    gram_start, cross_start = states
    queries, key_rows, value_rows, log_rates, gate_rows = inputs
    q_heads = jnp.transpose(queries, (1, 0, 2))
    k_heads = jnp.transpose(key_rows, (1, 0, 2))
    v_heads = jnp.transpose(value_rows, (1, 0, 2))
    cumulative = jnp.transpose(jnp.cumsum(log_rates, axis=0))
    length = cumulative.shape[1]
    causal = (jnp.arange(length)[:, None] >= jnp.arange(length)[None, :])[None]
    distance = cumulative[:, :, None] - cumulative[:, None, :]
    decay_mix = (
        jnp.where(causal, jnp.exp(jnp.where(causal, distance, 0.0)), 0.0)
        * jnp.transpose(gate_rows)[:, None, :]
    )
    start_scale = jnp.exp(cumulative)[:, :, None]
    iterate = jnp.zeros_like(q_heads)
    remain = q_heads
    search = q_heads
    norm_now = jnp.sum(remain * remain, axis=-1, keepdims=True)
    for sweep_index in range(CG_ITERS):
        carried = start_scale * jnp.einsum("hcd,hed->hce", search, gram_start, precision=exact_mode)
        operator_products = jnp.einsum("hjd,hid->hji", search, k_heads, precision=exact_mode)
        local_part = jnp.einsum(
            "hji,hid->hjd", decay_mix * operator_products, k_heads, precision=exact_mode
        )
        image_vec = carried + local_part + ridge_diag[:, None, :] * search
        step_size = norm_now / (jnp.sum(search * image_vec, axis=-1, keepdims=True) + 1e-06)
        iterate = iterate + step_size * search
        remain = remain - step_size * image_vec
        norm_next = jnp.sum(remain * remain, axis=-1, keepdims=True)
        search = remain + norm_next / (norm_now + 1e-06) * search
        norm_now = norm_next
    products = jnp.einsum("hjd,hid->hji", iterate, k_heads, precision=exact_mode)
    mesa_rows = start_scale * jnp.einsum("hje,hde->hjd", iterate, cross_start, precision=exact_mode)
    mesa_rows = mesa_rows + jnp.einsum(
        "hji,hid->hjd", decay_mix * products, v_heads, precision=exact_mode
    )
    tail_weight = (jnp.exp(cumulative[:, -1:] - cumulative) * jnp.transpose(gate_rows))[:, :, None]
    end_scale = jnp.exp(cumulative[:, -1])[:, None, None]
    gram_end = end_scale * gram_start + jnp.einsum(
        "hid,hie->hde", k_heads * tail_weight, k_heads, precision=exact_mode
    )
    cross_end = end_scale * cross_start + jnp.einsum(
        "hid,hie->hde", v_heads * tail_weight, k_heads, precision=exact_mode
    )
    return ((gram_end, cross_end), jnp.transpose(mesa_rows, (1, 0, 2)))


def mesa_pass(
    queries, key_rows, value_rows, log_rates, gate_rows, ridge_diag, gram_start, cross_start
):
    row_total = queries.shape[0]
    span_count = row_total // SPAN

    def shaped(array_in):
        return array_in.reshape((span_count, SPAN) + array_in.shape[1:])

    def advance(states, inputs):
        return span_update(states, inputs, ridge_diag)

    finished, outputs = lax.scan(
        advance,
        (gram_start, cross_start),
        (
            shaped(queries),
            shaped(key_rows),
            shaped(value_rows),
            shaped(log_rates),
            shaped(gate_rows),
        ),
    )
    return outputs.reshape(row_total, -1)


def fold_block(state_now, queries, key_value, query_first, key_first):
    running_max, running_sum, weighted = state_now
    row_count, head_count, head_size = queries.shape
    key_rows = key_value[0].reshape(-1, head_count, head_size)
    value_rows = key_value[1].reshape(-1, head_count, head_size)
    scores = jnp.einsum(
        "qhd,khd->hqk", queries, key_rows, preferred_element_type=jnp.float32
    ) * head_size ** (-0.5)
    query_pos = query_first + jnp.arange(row_count, dtype=jnp.int32)[:, None]
    key_pos = key_first + jnp.arange(key_rows.shape[0], dtype=jnp.int32)[None, :]
    distance = query_pos - key_pos
    inside = ((distance >= 0) & (distance < WINDOW) & (key_pos >= 0))[None]
    scores = jnp.where(inside, scores, masked_score)
    new_max = jnp.maximum(running_max, jnp.max(scores, axis=-1))
    weights = jnp.exp(scores - new_max[:, :, None]) * inside.astype(jnp.float32)
    rescale = jnp.exp(running_max - new_max)
    running_sum = running_sum * rescale + jnp.sum(weights, axis=-1)
    weighted = weighted * rescale[:, :, None] + jnp.einsum(
        "hqk,khd->hqd", weights.astype(jnp.bfloat16), value_rows, preferred_element_type=jnp.float32
    )
    return (new_max, running_sum, weighted)


def combine_pair(earlier, later):
    return (earlier[0] + later[0], jnp.exp(later[0])[:, None, None] * earlier[1] + later[1])


def split_cat(value, axis):
    high = value.astype(jnp.bfloat16)
    low = (value - high.astype(jnp.float32)).astype(jnp.bfloat16)
    return jnp.concatenate([high, low], axis=axis)


def dot_nn(a, b):
    return lax.dot_general(a, b, (((1,), (0,)), ((), ())), preferred_element_type=jnp.float32)


def dot_nt(a, b):
    return lax.dot_general(a, b, (((1,), (1,)), ((), ())), preferred_element_type=jnp.float32)


def fresh_state(packed, others):
    rows = others.shape[0]
    keys = packed[:rows].astype(jnp.float32)
    extra = packed[rows:].astype(jnp.float32)
    count = rows // packed.shape[1]
    weights = extra[:count] + extra[count : 2 * count]
    weights = jnp.concatenate([weights[c : c + 1] for c in range(count)], axis=1)
    decay = extra[2 * count : 2 * count + 1] + extra[2 * count + 1 : 2 * count + 2]
    weighted = split_cat(jnp.transpose(keys) * weights, 1)
    return decay, dot_nn(weighted, jnp.concatenate([others, others], axis=0))


def pack_keys_kernel(k_ref, rate_ref, gate_ref, out_ref, total_ref):
    heads, height, size = out_ref.shape
    rows = k_ref.shape[0]
    count = rows // size
    at = lax.broadcasted_iota(jnp.int32, (rows, rows), 0)
    upper = (at <= lax.broadcasted_iota(jnp.int32, (rows, rows), 1)).astype(jnp.float32)
    totals = lax.dot_general(
        rate_ref[...],
        upper,
        (((1,), (0,)), ((), ())),
        precision=exact_mode,
        preferred_element_type=jnp.float32,
    )
    gates = gate_ref[...]
    total_ref[...] = totals
    last = totals[:, rows - 1 :]
    weights = jnp.exp(last - totals) * gates
    decays = jnp.broadcast_to(jnp.exp(last), (heads, size))
    place = lax.broadcasted_iota(jnp.int32, (height - rows, size), 0)
    for h in range(heads):
        pieces = [weights[h : h + 1, c * size : (c + 1) * size] for c in range(count)]
        high = [p.astype(jnp.bfloat16).astype(jnp.float32) for p in pieces]
        decay = decays[h : h + 1]
        decay_high = decay.astype(jnp.bfloat16).astype(jnp.float32)
        lines = high + [p - q for p, q in zip(pieces, high)] + [decay_high, decay - decay_high]
        tile = jnp.zeros((height - rows, size), jnp.float32)
        for n, line in enumerate(lines):
            tile = jnp.where(place == n, line, tile)
        out_ref[h, :rows, :] = k_ref[:, h * size : (h + 1) * size]
        out_ref[h, rows:, :] = tile.astype(jnp.bfloat16)


def pack_keys(keys, rates, gates, size):
    rows, features = keys.shape
    heads = features // size
    spare = -(-(2 * (rows // size) + 2) // 16) * 16
    small = jax.ShapeDtypeStruct((heads, rows), jnp.float32)
    return pl.pallas_call(
        pack_keys_kernel,
        out_shape=[
            jax.ShapeDtypeStruct((heads, rows + spare, size), jnp.bfloat16),
            small,
        ],
        name="pack_keys",
    )(keys, rates, gates)


def attend_kernel(qkv_ref, key_ref, out_ref, state_ref, *, rows, reach):
    i = pl.program_id(0)
    size = qkv_ref.shape[-1]
    factor = size ** (-0.5) * math.log2(math.e)
    col = lax.broadcasted_iota(jnp.int32, (rows, rows), 1)
    row = lax.broadcasted_iota(jnp.int32, (rows, rows), 0)

    def run(first, count, full):
        q = qkv_ref[i, pl.ds(0, rows), :]
        scores = []
        for c in range(count):
            s = dot_nt(q, qkv_ref[first + c, pl.ds(rows, rows), :])
            if full:
                if c == 0:
                    s = jnp.where(col > row, s, masked_score)
                elif c == count - 1:
                    s = jnp.where(col <= row, s, masked_score)
            else:
                s = jnp.where(col - row <= (i - c) * rows, s, masked_score)
            scores.append(s)
        top = jnp.max(functools.reduce(jnp.maximum, scores), axis=-1, keepdims=True)
        total = None
        acc = None
        for c in range(count):
            w = jnp.exp2((scores[c] - top) * factor)
            part = dot_nn(w.astype(jnp.bfloat16), qkv_ref[first + c, pl.ds(2 * rows, rows), :])
            total = w if total is None else total + w
            acc = part if acc is None else acc + part
        total = jnp.sum(total, axis=-1, keepdims=True)
        value = (acc / total).astype(out_ref.dtype)
        out_ref[0, :rows, :] = value
        decay, fresh = fresh_state(key_ref[i], value)
        state = state_ref[...]
        out_ref[0, rows:, :] = state.astype(out_ref.dtype)
        state_ref[...] = decay * state + fresh

    @pl.when(i == 0)
    def _():
        state_ref[...] = jnp.zeros_like(state_ref)

    bounds = sorted({max(1, reach * n // 4) for n in range(1, 5)})
    low = 0
    for bound in bounds:
        pl.when((i >= low) & (i < bound))(functools.partial(run, 0, bound, False))
        low = bound
    pl.when(i >= reach)(lambda: run(i - reach, reach + 1, True))


def attend(qkv, keys, rows, reach):
    slabs, _, size = qkv.shape
    return pl.pallas_call(
        functools.partial(attend_kernel, rows=rows, reach=reach),
        grid=(slabs,),
        in_specs=[
            pl.BlockSpec(qkv.shape, lambda i: (0, 0, 0)),
            pl.BlockSpec(keys.shape, lambda i: (0, 0, 0)),
        ],
        out_specs=pl.BlockSpec((1, rows + size, size), lambda i: (i, 0, 0)),
        out_shape=jax.ShapeDtypeStruct((slabs, rows + size, size), jnp.bfloat16),
        scratch_shapes=[pltpu.VMEM((size, size), jnp.float32)],
        name="attend",
    )(qkv, keys)


def grams_kernel(k_ref, out_ref, *, rows):
    slabs, _, size = k_ref.shape
    state = jnp.zeros((size, size), jnp.float32)
    for j in range(slabs):
        out_ref[j] = state.astype(out_ref.dtype)
        if j < slabs - 1:
            decay, fresh = fresh_state(k_ref[j], k_ref[j, :rows, :])
            state = decay * state + fresh


def grams(keys, rows):
    slabs, _, size = keys.shape
    return pl.pallas_call(
        functools.partial(grams_kernel, rows=rows),
        out_shape=jax.ShapeDtypeStruct((slabs, size, size), jnp.bfloat16),
        name="grams",
    )(keys)


def solve_kernel(q_ref, k_ref, rate_ref, gate_ref, ridge_ref, gram_ref, x_ref, p_ref):
    rows = q_ref.shape[0]
    heads, size = ridge_ref.shape[1:]
    causal = lax.broadcasted_iota(jnp.int32, (rows, rows), 0) >= lax.broadcasted_iota(
        jnp.int32, (rows, rows), 1
    )
    held = []
    for h in range(heads):
        cols = slice(h * size, (h + 1) * size)
        key = k_ref[:, cols]
        by_col = jnp.broadcast_to(rate_ref[0, h : h + 1, :], (rows, rows))
        by_row = jnp.transpose(by_col)
        mix = (
            jnp.where(causal, jnp.exp(jnp.where(causal, by_row - by_col, 0.0)), 0.0)
            * gate_ref[0, h : h + 1, :]
        )
        gram = gram_ref[h]
        query = q_ref[:, cols].astype(jnp.float32)
        held.append(
            dict(
                wide=jnp.concatenate([key, key], axis=1),
                tall=jnp.concatenate([key, key], axis=0),
                gram=jnp.concatenate([gram, gram], axis=0),
                mix=mix,
                scale=jnp.exp(by_row[:, :size]),
                ridge=ridge_ref[0, h : h + 1, :],
                x=jnp.zeros_like(query),
                r=query,
                p=query,
                rr=jnp.sum(query * query, axis=-1, keepdims=True),
            )
        )
    for _ in range(CG_ITERS):
        for s in held:
            p = s["p"]
            parts = split_cat(p, 1)
            products = split_cat(s["mix"] * dot_nt(parts, s["wide"]), 1)
            image = (
                s["scale"] * dot_nn(parts, s["gram"]) + dot_nn(products, s["tall"]) + s["ridge"] * p
            )
            alpha = s["rr"] / (jnp.sum(p * image, axis=-1, keepdims=True) + 1e-6)
            s["x"] = s["x"] + alpha * p
            s["r"] = s["r"] - alpha * image
            new = jnp.sum(s["r"] * s["r"], axis=-1, keepdims=True)
            s["p"] = s["r"] + (new / (s["rr"] + 1e-6)) * p
            s["rr"] = new
    for h, s in enumerate(held):
        x_ref[h] = (s["scale"] * s["x"]).astype(x_ref.dtype)
        p_ref[h] = (s["mix"] * dot_nt(split_cat(s["x"], 1), s["wide"])).astype(p_ref.dtype)


def solve(queries, keys, rates, gates, ridge, gram, group):
    rows = queries.shape[0]
    heads, size = ridge.shape
    steps = heads // group

    def packed(a):
        return a.reshape(steps, group, a.shape[-1])

    def small(width):
        return pl.BlockSpec((1, group, width), lambda i: (i, 0, 0))

    wide = pl.BlockSpec((rows, group * size), lambda i: (0, i))
    return pl.pallas_call(
        solve_kernel,
        grid=(steps,),
        in_specs=[
            wide,
            wide,
            small(rows),
            small(rows),
            small(size),
            pl.BlockSpec((group, size, size), lambda i: (i, 0, 0)),
        ],
        out_specs=[
            pl.BlockSpec((group, rows, size), lambda i: (i, 0, 0)),
            pl.BlockSpec((group, rows, rows), lambda i: (i, 0, 0)),
        ],
        out_shape=[
            jax.ShapeDtypeStruct((heads, rows, size), jnp.bfloat16),
            jax.ShapeDtypeStruct((heads, rows, rows), jnp.bfloat16),
        ],
        name="solve",
    )(queries, keys, packed(rates), packed(gates), packed(ridge), gram)


def finish_kernel(x_ref, p_ref, back_ref, att_ref, out_ref):
    heads, rows, size = x_ref.shape
    for h in range(heads):
        cols = slice(h * size, (h + 1) * size)
        value = back_ref[h, :rows, :]
        att_ref[:, cols] = value
        out_ref[:, cols] = (dot_nn(x_ref[h], back_ref[h, rows:, :]) + dot_nn(p_ref[h], value)).astype(
            out_ref.dtype
        )


def finish(x, products, back, group):
    heads, rows, size = x.shape

    def spec(a):
        return pl.BlockSpec((group,) + a.shape[1:], lambda i: (i, 0, 0))

    flat = pl.BlockSpec((rows, group * size), lambda i: (0, i))
    shape = jax.ShapeDtypeStruct((rows, heads * size), jnp.bfloat16)
    return pl.pallas_call(
        finish_kernel,
        grid=(heads // group,),
        in_specs=[spec(x), spec(products), spec(back)],
        out_specs=[flat, flat],
        out_shape=[shape, shape],
        name="finish",
    )(x, products, back)


def exchange(value):
    return lax.all_to_all(value, "seq", 0, 0, tiled=True)


def by_head(value, heads):
    rows = value.shape[0]
    return jnp.transpose(value.reshape(rows, heads, -1), (1, 0, 2))


def head_body(
    attn_query, attn_key, attn_value, mesa_query, mesa_key, log_decay, input_gate, regularizer
):
    rows = attn_query.shape[0]
    heads, size = regularizer.shape
    gates = jnp.transpose(input_gate)
    packed, rates = pack_keys(mesa_key, jnp.transpose(log_decay), gates, size)
    keys = exchange(packed)
    qkv = exchange(
        jnp.concatenate([by_head(a, heads) for a in (attn_query, attn_key, attn_value)], axis=1)
    )
    gram = exchange(grams(keys, rows))
    back = exchange(attend(qkv, keys, rows, WINDOW // rows))
    group = math.gcd(heads, 4)
    x, products = solve(mesa_query, mesa_key, rates, gates, regularizer, gram, group)
    return tuple(finish(x, products, back, math.gcd(heads, 8)))


def body(
    attn_query, attn_key, attn_value, mesa_query, mesa_key, log_decay, input_gate, regularizer
):
    row_count = attn_query.shape[0]
    head_count, head_size = regularizer.shape
    shape3 = (row_count, head_count, head_size)
    slab_first = lax.axis_index("seq") * row_count
    keys_float = mesa_key.astype(jnp.float32).reshape(shape3)
    slab_log = jnp.sum(log_decay, axis=0)
    tail_log = slab_log[None, :] - jnp.cumsum(log_decay, axis=0)
    weight_rows = (jnp.exp(tail_log) * input_gate)[:, :, None]
    gram_local = jnp.einsum(
        "lhd,lhe->hde", keys_float * weight_rows, keys_float, precision=exact_mode
    )
    zero_log = jnp.zeros_like(slab_log)
    zero_state = jnp.zeros_like(gram_local)
    gram_prefix = prefix((slab_log, gram_local), "seq", combine_pair, (zero_log, zero_state))[1]
    queries = attn_query.reshape(shape3)
    key_value = jnp.stack([attn_key, attn_value])
    state_now = (
        jnp.full((head_count, row_count), masked_score, jnp.float32),
        jnp.zeros((head_count, row_count), jnp.float32),
        jnp.zeros((head_count, row_count, head_size), jnp.float32),
    )
    state_now = fold_block(state_now, queries, key_value, slab_first, slab_first)
    reach = -(-WINDOW // row_count)
    moving = key_value
    for hop_index in range(1, reach + 1):
        moving = passed_along(moving, "seq", 1)
        state_now = fold_block(
            state_now, queries, moving, slab_first, slab_first - hop_index * row_count
        )
    normed = state_now[2] / state_now[1][:, :, None]
    attention = jnp.transpose(normed, (1, 0, 2)).reshape(row_count, -1).astype(jnp.bfloat16)
    values_float = attention.astype(jnp.float32).reshape(shape3)
    cross_local = jnp.einsum(
        "lhd,lhe->hde", values_float * weight_rows, keys_float, precision=exact_mode
    )
    cross_prefix = prefix((slab_log, cross_local), "seq", combine_pair, (zero_log, zero_state))[1]
    mesa_out = mesa_pass(
        mesa_query.astype(jnp.float32).reshape(shape3),
        keys_float,
        values_float,
        log_decay,
        input_gate,
        regularizer,
        gram_prefix,
        cross_prefix,
    )
    return (attention, mesa_out.astype(jnp.bfloat16))


def solution(mesh):
    def chosen(*arrays):
        rows = arrays[0].shape[0]
        heads, size = arrays[-1].shape
        fits = WINDOW % rows == 0 and rows % 128 == 0 and size == 128
        if heads == mesh.shape["seq"] and fits:
            return head_body(*arrays)
        return body(*arrays)

    return jax.shard_map(
        chosen,
        mesh=mesh,
        in_specs=(
            P(("groups", "seq"), None),
            P(("groups", "seq"), None),
            P(("groups", "seq"), None),
            P(("groups", "seq"), None),
            P(("groups", "seq"), None),
            P(("groups", "seq"), None),
            P(("groups", "seq"), None),
            P(),
        ),
        out_specs=(P(("groups", "seq"), None), P(("groups", "seq"), None)),
        check_vma=False,
    )
```
